32 devices in a mesh: fsdp: 8 (over z, y), ctx: 2 (over core), tp: 2 (over x).
Axes of the slice: x: 2, y: 2, z: 4, core: 2. Of those that a mesh axis runs over, the one named last changes fastest.
Arguments:
- tokens: bfloat16 [8192, 2048], P(('fsdp', 'ctx')), may hold values from -6 to 6
- segments: int32 [8, 1024], P('fsdp'), may hold values from 0 to 7, never falling along the last dimension, each value on 1 to 512 neighbouring positions
- cotangent: bfloat16 [8192, 2048], P(('fsdp', 'ctx')), may hold values from -6 to 6
- gain_attn: bfloat16 [2048], P('fsdp'), may hold values from 0.5 to 1.5
- w_query: bfloat16 [2048, 2048], P('fsdp', 'tp'), may hold values from -0.125 to 0.125
- w_key: bfloat16 [2048, 256], P('fsdp', 'tp'), may hold values from -0.125 to 0.125
- w_value: bfloat16 [2048, 256], P('fsdp', 'tp'), may hold values from -0.125 to 0.125
- w_output: bfloat16 [2048, 2048], P('tp', 'fsdp'), may hold values from -0.75 to 0.75
- gain_mlp: bfloat16 [2048], P('fsdp'), may hold values from 0.5 to 1.5
- w_gate: bfloat16 [2048, 5632], P('fsdp', 'tp'), may hold values from -0.125 to 0.125
- w_up: bfloat16 [2048, 5632], P('fsdp', 'tp'), may hold values from -0.125 to 0.125
- w_down: bfloat16 [5632, 2048], P('tp', 'fsdp'), may hold values from -0.078125 to 0.078125
Outputs:
- output: bfloat16 [8192, 2048], P(('fsdp', 'ctx'))
- input_grad: float32 [8192, 2048], P(('fsdp', 'ctx'))
- grad_gain_attn: float32 [2048], P(('fsdp', 'ctx'))
- grad_query: float32 [2048, 2048], P(('fsdp', 'ctx'), 'tp')
- grad_key: float32 [2048, 256], P(('fsdp', 'ctx'), 'tp')
- grad_value: float32 [2048, 256], P(('fsdp', 'ctx'), 'tp')
- grad_output: float32 [2048, 2048], P('tp', ('fsdp', 'ctx'))
- grad_gain_mlp: float32 [2048], P(('fsdp', 'ctx'))
- grad_gate: float32 [2048, 5632], P(('fsdp', 'ctx'), 'tp')
- grad_up: float32 [2048, 5632], P(('fsdp', 'ctx'), 'tp')
- grad_down: float32 [5632, 2048], P('tp', ('fsdp', 'ctx'))
The draws below stay inside these ranges and needn't reach their ends.
Inputs may be any that keep to these rules, and one draw needn't show every extreme that they name: `segments`: along each sequence the document numbers never fall; each document has 1 to 512 positions and one of each sequence has exactly 512.
All inputs are finite; a program needn't handle non-finite values.
Results may differ from the reference program's by a relative error of at most 0.014.
Values may be sent and summed in bfloat16 or wider, within the bound.
A program may use at most 256 MiB of HBM per device.

```python
import math
import jax
import jax.numpy as jnp
import numpy as np
from jax import lax

D = 2048
HEADS = 32
KV = 4
HD = 64
FF = 5632
SEQ = 1024
SEQS = 8
TOKENS = 8192
DOCS = 8
LONGEST = 512


def block_scale(rng, shape, cuts, smallest, largest):
    loudness, own = 1.0, jax.random.fold_in(rng, 6)
    for axis_at, blocks in cuts:
        draws = jnp.exp(jax.random.uniform(jax.random.fold_in(own, axis_at), (blocks,), jnp.float32, smallest / len(cuts), largest / len(cuts)))
        loudness = loudness * jnp.repeat(draws, shape[axis_at] // blocks).reshape([-1 if axis == axis_at else 1 for axis in range(len(shape))])
    return loudness


def split_up(amount, total, most, slope):
    loads = [(1 << 20) // math.isqrt(rank ** slope) + 1 for rank in range(2, amount + 1)]
    surplus, holding = total - most - (amount - 1), [1] * (amount - 1)
    while surplus > 0:
        movable = [i for i in range(amount - 1) if holding[i] < most]
        pool, remaining = sum([loads[i] for i in movable]), surplus
        for i in movable:
            addition = min(most - holding[i], max(1, remaining * loads[i] // pool), surplus)
            holding[i] = holding[i] + addition
            surplus = surplus - addition
    return np.array([most] + holding)


def uneven(stream_key, amount, total, limit, skew):
    if amount == 2:
        one = jax.random.randint(stream_key, (), max(1, total - limit), min(limit, total - 1) + 1)
        return jnp.stack([one, total - one])
    tallies = jnp.asarray(split_up(amount, total, limit, skew), jnp.int32)
    twos = (amount - 1) // 2
    source_of, sink = tallies[1:1 + 2 * twos:2], tallies[2:2 + 2 * twos:2]
    room = jnp.minimum(source_of - 1, limit - sink)
    passed = jax.random.randint(jax.random.fold_in(stream_key, 1), (twos,), 0, 1 << 20) % (room + 1)
    tallies = tallies.at[1:1 + 2 * twos:2].set(source_of - passed).at[2:2 + 2 * twos:2].set(sink + passed)
    return tallies[jax.random.permutation(jax.random.fold_in(stream_key, 2), amount)]


def scatter_about(key, extent, deviation, most, cuts=(), kind=jnp.bfloat16):
    drawn = deviation * jax.random.normal(key, extent, jnp.float32)
    if cuts:
        drawn = drawn * block_scale(key, extent, cuts, -0.22, 0.18)
    return jnp.clip(drawn, -most, most).astype(kind)


def setup_inputs(seed: int = 0) -> dict:
    key_list = jax.random.split(jax.random.key(seed), 13)
    return {
        "tokens": scatter_about(key_list[0], (TOKENS, D), 1.0, 6.0, ((0, 16),)),
        "segments": jax.vmap(lambda own: jnp.searchsorted(jnp.cumsum(uneven(own, DOCS, SEQ, LONGEST, 2)), jnp.arange(SEQ), side="right"))(jax.random.split(key_list[1], SEQS)).reshape((SEQS, SEQ)).astype(jnp.int32),
        "cotangent": scatter_about(key_list[2], (TOKENS, D), 1.0, 6.0, ((0, 16),)),
        "gain_attn": jnp.clip(1.0 + 0.1 * jax.random.normal(key_list[3], (D,), jnp.float32), 0.5, 1.5).astype(jnp.bfloat16),
        "w_query": scatter_about(key_list[4], (D, HEADS * HD), D ** -0.5, 0.125, ((0, 8), (1, 2))),
        "w_key": scatter_about(key_list[5], (D, KV * HD), D ** -0.5, 0.125, ((0, 8), (1, 2))),
        "w_value": scatter_about(key_list[6], (D, KV * HD), D ** -0.5, 0.125, ((0, 8), (1, 2))),
        "w_output": scatter_about(key_list[7], (HEADS * HD, D), (D // 32) ** -0.5, 0.75, ((0, 2), (1, 8))),
        "gain_mlp": jnp.clip(1.0 + 0.1 * jax.random.normal(key_list[8], (D,), jnp.float32), 0.5, 1.5).astype(jnp.bfloat16),
        "w_gate": scatter_about(key_list[9], (D, FF), D ** -0.5, 0.125, ((0, 8), (1, 2))),
        "w_up": scatter_about(key_list[10], (D, FF), D ** -0.5, 0.125, ((0, 8), (1, 2))),
        "w_down": scatter_about(key_list[11], (FF, D), FF ** -0.5, 0.078125, ((0, 2), (1, 8))),
    }


@jax.custom_vjp
def low(v):
    return lax.optimization_barrier(v.astype(jnp.bfloat16)).astype(jnp.float32)

@jax.custom_vjp
def low_back(v):
    return v

def low_keep(v):
    return (low(v), None)

def low_pass(kept, grad):
    return (grad,)

def back_keep(v):
    return (v, None)

def back_low(kept, grad):
    return (low(grad),)
low.defvjp(low_keep, low_pass)
low_back.defvjp(back_keep, back_low)

def matmul(left, right):
    return jnp.dot(left, right, precision=lax.Precision.HIGHEST)

def inverse_rms(values):
    return lax.rsqrt(lax.optimization_barrier(jnp.mean(values * values, axis=-1, keepdims=True)) + 1e-05)

def rotary_tables(count):
    half_dim = HD // 2
    places = jnp.arange(count).astype(jnp.float32)
    freqs = jnp.power(jnp.float32(10000.0), -(2.0 * jnp.arange(half_dim).astype(jnp.float32)) / HD)
    angles = places[:, None] * freqs[None, :]
    return (jnp.cos(angles), jnp.sin(angles))

def rotate(values, cosine, sine_table):
    half_dim = values.shape[-1] // 2
    first_half = values[..., :half_dim]
    second_half = values[..., half_dim:]
    cos_rows = cosine[:, None, :]
    sin_rows = sine_table[:, None, :]
    return jnp.concatenate([first_half * cos_rows - second_half * sin_rows, second_half * cos_rows + first_half * sin_rows], axis=-1)

def attention(queries, key_rows, value_rows, seg_row):
    count = queries.shape[0]
    tile_rows = min(512, count)
    group_size = HEADS // KV
    score_scale = 1.0 / math.sqrt(HD)
    query_tiles = queries.reshape(count // tile_rows, tile_rows, KV, group_size, HD)
    positions = jnp.arange(count).astype(jnp.int32)

    def one_tile(pieces):
        query_tile, seg_tile, pos_tile = pieces
        scores = jnp.einsum('rkgd,skd->kgrs', query_tile, key_rows, precision=lax.Precision.HIGHEST) * score_scale
        scores = low_back(scores)
        allowed = (seg_tile[:, None] == seg_row[None, :]) & (positions[None, :] <= pos_tile[:, None])
        scores = jnp.where(allowed[None, None], scores, -1e+30)
        row_max = lax.optimization_barrier(jnp.max(scores, axis=-1, keepdims=True))
        expo = jnp.exp(scores - row_max)
        probabilities = low(expo / lax.optimization_barrier(jnp.sum(expo, axis=-1, keepdims=True)))
        return jnp.einsum('kgrs,skd->rkgd', probabilities, value_rows, precision=lax.Precision.HIGHEST)
    mixed = lax.map(jax.checkpoint(one_tile), (query_tiles, seg_row.reshape(-1, tile_rows), positions.reshape(-1, tile_rows)))
    return low(low_back(mixed.reshape(count, HEADS * HD)))

def whole_layer(inputs, params, seg_row):
    gain_one, query_w, key_w, value_w, output_w, gain_two, gate_w, up_w, down_w = params
    count = inputs.shape[0]
    hidden_one = low(inputs * inverse_rms(inputs) * gain_one)
    cosine, sine_table = rotary_tables(count)
    queries = low(rotate(low_back(matmul(hidden_one, query_w)).reshape(count, HEADS, HD), cosine, sine_table))
    key_rows = low(rotate(low_back(matmul(hidden_one, key_w)).reshape(count, KV, HD), cosine, sine_table))
    value_rows = low(low_back(matmul(hidden_one, value_w))).reshape(count, KV, HD)
    attended = attention(queries, key_rows, value_rows, seg_row)
    residual = inputs + low_back(matmul(attended, output_w))
    hidden_two = low(residual * inverse_rms(residual) * gain_two)
    gate_rows = low_back(matmul(hidden_two, gate_w))
    up_rows = low_back(matmul(hidden_two, up_w))
    inner_rows = low(jax.nn.silu(gate_rows) * up_rows)
    return residual + low_back(matmul(inner_rows, down_w))

def reference(tokens, segments, cotangent, gain_attn, w_query, w_key, w_value, w_output, gain_mlp, w_gate, w_up, w_down):
    weights = tuple((item.astype(jnp.float32) for item in (gain_attn, w_query, w_key, w_value, w_output, gain_mlp, w_gate, w_up, w_down)))
    sequences = tokens.astype(jnp.float32).reshape(SEQS, SEQ, D)
    cotangents = cotangent.astype(jnp.float32).reshape(SEQS, SEQ, D)

    def one_sequence(totals, pieces):
        inputs, seg_row, upstream = pieces
        result, pullback = jax.vjp(lambda values, *params: whole_layer(values, params, seg_row), inputs, *weights)
        gradients = pullback(upstream)
        totals = tuple((first + second for first, second in zip(totals, gradients[1:])))
        return (totals, (result.astype(jnp.bfloat16), gradients[0]))
    zeros = tuple((jnp.zeros_like(item) for item in weights))
    totals, (results, input_grads) = lax.scan(one_sequence, zeros, (sequences, segments, cotangents))
    return (results.reshape(TOKENS, D), input_grads.reshape(TOKENS, D), totals[0], totals[1], totals[2], totals[3], totals[4], totals[5], totals[6], totals[7], totals[8])
```

```python
import math

import jax
import jax.numpy as jnp
from jax import lax
from jax.sharding import PartitionSpec as P

HD = 64
BF = jnp.bfloat16
F32 = jnp.float32


def dot(a, b, ca, cb, out=F32):
    return lax.dot_general(a, b, (((ca,), (cb,)), ((), ())), preferred_element_type=F32).astype(out)


def inverse_rms(values):
    return lax.rsqrt(jnp.mean(values * values, axis=-1, keepdims=True) + 1e-05)


def rotary_tables(first_row, count):
    half_dim = HD // 2
    places = (first_row + jnp.arange(count, dtype=jnp.int32)).astype(F32)
    freqs = jnp.power(F32(10000.0), -(2.0 * jnp.arange(half_dim).astype(F32)) / HD)
    angles = places[:, None] * freqs[None, :]
    return (jnp.cos(angles), jnp.sin(angles))


def rotate(values, cosine, sine_table):
    half_dim = values.shape[-1] // 2
    first_half = values[..., :half_dim]
    second_half = values[..., half_dim:]
    cos_rows = cosine[:, None, :]
    sin_rows = sine_table[:, None, :]
    return jnp.concatenate(
        [
            first_half * cos_rows - second_half * sin_rows,
            second_half * cos_rows + first_half * sin_rows,
        ],
        axis=-1,
    )


def make_mask(query_seg, query_pos, key_seg, key_pos, live_flag):
    return (
        (query_seg[:, None] == key_seg[None, :])
        & (key_pos[None, :] <= query_pos[:, None])
        & live_flag
    )


def block_scores(query_tile, key_block, allowed, score_scale):
    raw_scores = (
        jnp.einsum("rkgd,skd->kgrs", query_tile, key_block, preferred_element_type=F32)
        * score_scale
    )
    return jnp.where(allowed[None, None], raw_scores, -1e30)


def attention_forward(queries, blocks, query_seg, query_pos):
    score_scale = 1.0 / math.sqrt(HD)
    length, groups, size, _ = queries.shape
    running_max = jnp.full((groups, size, length), -1e30, F32)
    running_sum = jnp.zeros((groups, size, length), F32)
    for keys, values, key_seg, key_pos, live in blocks:
        allowed = make_mask(query_seg, query_pos, key_seg, key_pos, live)
        scores = block_scores(queries, keys, allowed, score_scale)
        new_max = jnp.maximum(running_max, jnp.max(scores, axis=-1))
        fresh = jnp.sum(
            jnp.where(allowed[None, None], jnp.exp(scores - new_max[..., None]), 0.0), axis=-1
        )
        running_sum = running_sum * jnp.exp(running_max - new_max) + fresh
        running_max = new_max
    log_total = running_max + jnp.log(running_sum)
    mixed = jnp.zeros((length, groups, size, HD), F32)
    for keys, values, key_seg, key_pos, live in blocks:
        allowed = make_mask(query_seg, query_pos, key_seg, key_pos, live)
        scores = block_scores(queries, keys, allowed, score_scale)
        probabilities = jnp.where(
            allowed[None, None], jnp.exp(scores - log_total[..., None]), 0.0
        ).astype(BF)
        mixed = mixed + jnp.einsum(
            "kgrs,skd->rkgd", probabilities, values, preferred_element_type=F32
        )
    return mixed.astype(BF), log_total


def attention_backward(queries, grads, log_total, blocks, query_seg, query_pos):
    score_scale = 1.0 / math.sqrt(HD)
    length, groups, size, _ = queries.shape
    delta_sum = jnp.zeros((groups, size, length), F32)
    for keys, values, key_seg, key_pos, live in blocks:
        allowed = make_mask(query_seg, query_pos, key_seg, key_pos, live)
        scores = block_scores(queries, keys, allowed, score_scale)
        probabilities = jnp.where(allowed[None, None], jnp.exp(scores - log_total[..., None]), 0.0)
        d_prob = jnp.einsum("rkgd,skd->kgrs", grads, values, preferred_element_type=F32)
        delta_sum = delta_sum + jnp.sum(probabilities * d_prob, axis=-1)
    d_query = jnp.zeros((length, groups, size, HD), F32)
    kv_grads = []
    for keys, values, key_seg, key_pos, live in blocks:
        allowed = make_mask(query_seg, query_pos, key_seg, key_pos, live)
        scores = block_scores(queries, keys, allowed, score_scale)
        probabilities = jnp.where(allowed[None, None], jnp.exp(scores - log_total[..., None]), 0.0)
        d_prob = jnp.einsum("rkgd,skd->kgrs", grads, values, preferred_element_type=F32)
        d_scores = (probabilities * (d_prob - delta_sum[..., None])).astype(BF)
        d_query = (
            d_query
            + jnp.einsum("kgrs,skd->rkgd", d_scores, keys, preferred_element_type=F32)
            * score_scale
        )
        d_key = (
            jnp.einsum("kgrs,rkgd->skd", d_scores, queries, preferred_element_type=F32)
            * score_scale
        )
        d_val = jnp.einsum(
            "kgrs,rkgd->skd", probabilities.astype(BF), grads, preferred_element_type=F32
        )
        kv_grads.append((d_key, d_val))
    return d_query, kv_grads


class Ring:
    def __init__(self):
        self.n = lax.axis_size("fsdp")
        self.m = self.n // 2
        self.place = lax.axis_index("fsdp")
        self.core = lax.axis_index("ctx")
        self.z, self.y = self.place // 2, self.place % 2

    def along_z(self, value, step):
        m = self.m
        pairs = [(z * 2 + y, ((z + step) % m) * 2 + y) for z in range(m) for y in range(2)]
        return lax.ppermute(value, "fsdp", pairs)

    def across_y(self, value):
        return lax.ppermute(value, "fsdp", [(i, i ^ 1) for i in range(self.n)])

    def across_core(self, value):
        return lax.ppermute(value, "ctx", [(0, 1), (1, 0)])

    def half(self, value, axis):
        size = value.shape[axis] // 2
        return lax.dynamic_slice_in_dim(value, self.core * size, size, axis)

    def relative(self, value):
        block = value.shape[1] // self.n
        parts = []
        for dy in range(2):
            for dz in range(self.m):
                at = ((self.z - dz + self.m) % self.m) * 2 + (self.y ^ dy)
                parts.append(lax.dynamic_slice_in_dim(value, at * block, block, 1))
        return jnp.concatenate(parts, axis=1)

    def absolute(self, value):
        block = value.shape[1] // self.n
        parts = []
        for at in range(self.n):
            dz = (self.z - at // 2 + self.m) % self.m
            dy = self.y ^ (at % 2)
            parts.append(lax.dynamic_slice_in_dim(value, (dy * self.m + dz) * block, block, 1))
        return jnp.concatenate(parts, axis=1)

    def gather(self, chunk):
        column = [chunk] + [self.along_z(chunk, step) for step in range(1, self.m)]
        near = jnp.concatenate(column, axis=0)
        far = self.across_y(near)
        return near, far

    def scatter(self, mine, theirs):
        block = mine.shape[0] // self.n
        total = (mine.astype(F32) + self.across_core(theirs).astype(F32)).astype(BF)
        rows = self.m * block
        column = (
            total[:rows].astype(F32) + self.across_y(total[rows:]).astype(F32)
        ).astype(BF)
        out = column[:block].astype(F32)
        for step in range(1, self.m):
            piece = column[step * block : (step + 1) * block]
            out = out + self.along_z(piece, -step).astype(F32)
        return out

    def settle(self, value):
        rows = value.shape[0] // 2
        keep = lax.dynamic_slice_in_dim(value, self.core * rows, rows, 0)
        give = lax.dynamic_slice_in_dim(value, (1 - self.core) * rows, rows, 0)
        return keep, self.across_core(give)

    def in_order(self, keep, got, axis):
        first = jnp.where(self.core == 0, keep, got)
        second = jnp.where(self.core == 0, got, keep)
        return jnp.concatenate([first, second], axis=axis)


def shared(partial):
    own = lax.reduce_precision(partial, 8, 7).astype(BF)
    other = lax.ppermute(own, "tp", [(0, 1), (1, 0)])
    return own.astype(F32) + other.astype(F32)


def shards(
    tokens,
    segments,
    cotangent,
    gain_attn,
    w_query,
    w_key,
    w_value,
    w_output,
    gain_mlp,
    w_gate,
    w_up,
    w_down,
):
    ring = Ring()
    length = tokens.shape[0]
    block = w_query.shape[0]
    first_row = ring.core * length
    cycle = lax.axis_size("ctx")

    q_half, k_half = w_query.shape[1] // 2, w_key.shape[1] // 2
    gains = jnp.zeros((16, q_half + 2 * k_half), BF)
    gains = gains.at[0, :block].set(gain_attn).at[1, :block].set(gain_mlp)
    own_qkv = jnp.concatenate(
        [
            jnp.concatenate([ring.half(w_query, 1), ring.half(w_key, 1), ring.half(w_value, 1)], 1),
            gains,
        ],
        axis=0,
    )
    near, far = ring.gather(own_qkv)
    both = jnp.concatenate([near, far], axis=0).reshape(ring.n, block + 16, q_half + 2 * k_half)
    qkv = [both[:, :block].reshape(ring.n * block, -1)]
    gain_one = both[:, block, :block].reshape(1, ring.n * block).astype(F32)
    gain_two = both[:, block + 1, :block].reshape(1, ring.n * block).astype(F32)
    qkv.append(ring.across_core(qkv[0]))

    def gathered(own):
        full = jnp.concatenate(ring.gather(own), axis=0)
        return [full, ring.across_core(full)]

    out_t = gathered(ring.half(w_output, 0).T)
    gate_w = gathered(ring.half(w_gate, 1))
    up_w = gathered(ring.half(w_up, 1))
    down_t = gathered(ring.half(w_down, 0).T)

    inputs = ring.relative(tokens).astype(F32)
    upstream = ring.relative(cotangent)
    inv_one = inverse_rms(inputs)
    normed_one = inputs * inv_one
    hidden_one = (normed_one * gain_one).astype(BF)
    cosine, sine_table = rotary_tables(first_row, length)
    queries, keys, values = [], [], []
    for part in range(2):
        pre = dot(hidden_one, qkv[part], 1, 0)
        pre_q = pre[:, :q_half].reshape(length, q_half // HD, HD)
        pre_k = pre[:, q_half : q_half + k_half].reshape(length, k_half // HD, HD)
        pre_v = pre[:, q_half + k_half :].reshape(length, k_half // HD, HD)
        queries.append(rotate(pre_q, cosine, sine_table).astype(BF))
        keys.append(rotate(pre_k, cosine, sine_table).astype(BF))
        values.append(pre_v.astype(BF))
    queries = jnp.stack(queries, axis=1)
    keys, values = jnp.concatenate(keys, axis=1), jnp.concatenate(values, axis=1)
    before = lax.ppermute(jnp.stack([keys, values]), "ctx", [(i, i + 1) for i in range(cycle - 1)])
    before = before[:, :, ::-1]

    seq_ids = segments[0]
    query_seg = lax.dynamic_slice_in_dim(seq_ids, first_row, length)
    query_pos = first_row + jnp.arange(length, dtype=jnp.int32)
    start_key = jnp.maximum(ring.core - 1, 0) * length
    key_seg = lax.dynamic_slice_in_dim(seq_ids, start_key, length)
    key_pos = start_key + jnp.arange(length, dtype=jnp.int32)
    blocks = [
        (keys, values, query_seg, query_pos, True),
        (before[0], before[1], key_seg, key_pos, ring.core > 0),
    ]
    attended, log_totals = attention_forward(queries, blocks, query_seg, query_pos)
    attn = [attended[:, part].reshape(length, q_half) for part in range(2)]
    residual = inputs + shared(dot(attn[0], out_t[0], 1, 1) + dot(attn[1], out_t[1], 1, 1))

    inv_two = inverse_rms(residual)
    normed_two = residual * inv_two
    hidden_two = (normed_two * gain_two).astype(BF)
    inner, d_gate, d_up = [], [], []
    for part in range(2):
        gate_rows = dot(hidden_two, gate_w[part], 1, 0)
        up_rows = dot(hidden_two, up_w[part], 1, 0)
        sigmoid_gate = jax.nn.sigmoid(gate_rows)
        swish = gate_rows * sigmoid_gate
        inner.append((swish * up_rows).astype(BF))
        d_inner = dot(upstream, down_t[part], 1, 0)
        d_gate.append(
            (d_inner * up_rows * sigmoid_gate * (1.0 + gate_rows * (1.0 - sigmoid_gate))).astype(BF)
        )
        d_up.append((d_inner * swish).astype(BF))
    grad_down_t = ring.scatter(*[dot(upstream, inner[part], 0, 0, BF) for part in range(2)])
    mlp_out = shared(dot(inner[0], down_t[0], 1, 1) + dot(inner[1], down_t[1], 1, 1))
    output = (residual + mlp_out).astype(BF)
    d_hidden_two = shared(
        dot(d_gate[0], gate_w[0], 1, 1)
        + dot(d_gate[1], gate_w[1], 1, 1)
        + dot(d_up[0], up_w[0], 1, 1)
        + dot(d_up[1], up_w[1], 1, 1)
    )
    grad_gate = ring.scatter(*[dot(hidden_two, d_gate[part], 0, 0, BF) for part in range(2)])
    grad_up = ring.scatter(*[dot(hidden_two, d_up[part], 0, 0, BF) for part in range(2)])
    scaled_two = d_hidden_two * gain_two
    grad_gain_two = jnp.sum(d_hidden_two * normed_two, axis=0)
    d_residual = upstream.astype(F32) + inv_two * (
        scaled_two - normed_two * jnp.mean(scaled_two * normed_two, axis=-1, keepdims=True)
    )

    d_branch = d_residual.astype(BF)
    grad_out_t = ring.scatter(*[dot(d_branch, attn[part], 0, 0, BF) for part in range(2)])
    d_attn = jnp.stack([dot(d_branch, out_t[part], 1, 0, BF) for part in range(2)], axis=1)
    d_query, kv_grads = attention_backward(
        queries, d_attn.reshape(queries.shape), log_totals, blocks, query_seg, query_pos
    )
    back = jnp.stack(kv_grads[1]).astype(BF)[:, :, ::-1]
    back = lax.ppermute(back, "ctx", [(i + 1, i) for i in range(cycle - 1)]).astype(F32)
    d_query_pre = rotate(
        d_query.reshape(length, -1, HD), cosine, -sine_table
    ).astype(BF).reshape(length, 2, q_half)
    d_key_pre = rotate(kv_grads[0][0] + back[0], cosine, -sine_table).astype(BF).reshape(length, 2, k_half)
    d_value_pre = (kv_grads[0][1] + back[1]).astype(BF).reshape(length, 2, k_half)
    d_qkv = [
        jnp.concatenate([d_query_pre[:, part], d_key_pre[:, part], d_value_pre[:, part]], axis=1)
        for part in range(2)
    ]
    grad_qkv = ring.scatter(*[dot(hidden_one, d_qkv[part], 0, 0, BF) for part in range(2)])
    d_hidden_one = shared(dot(d_qkv[0], qkv[0], 1, 1) + dot(d_qkv[1], qkv[1], 1, 1))
    scaled_one = d_hidden_one * gain_one
    grad_gain_one = jnp.sum(d_hidden_one * normed_one, axis=0)
    d_input = d_residual + inv_one * (
        scaled_one - normed_one * jnp.mean(scaled_one * normed_one, axis=-1, keepdims=True)
    )

    both_gains = jnp.stack([grad_gain_one, grad_gain_two]).reshape(2, ring.n, block)
    both_gains = both_gains + ring.across_core(both_gains)
    near = both_gains[:, : ring.m] + ring.across_y(both_gains[:, ring.m :])
    gain_sum = near[:, 0]
    for step in range(1, ring.m):
        gain_sum = gain_sum + ring.along_z(near[:, step], -step)
    gain_sum = ring.half(gain_sum, 1)

    def finish(value):
        return ring.in_order(*ring.settle(value), 1)

    keep, got = ring.settle(grad_qkv)
    cut = [(0, q_half), (q_half, q_half + k_half), (q_half + k_half, q_half + 2 * k_half)]
    grad_query, grad_key, grad_value = [
        ring.in_order(keep[:, low:high], got[:, low:high], 1) for low, high in cut
    ]
    return (
        ring.absolute(output),
        ring.absolute(d_input),
        gain_sum[0],
        grad_query,
        grad_key,
        grad_value,
        finish(grad_out_t).T,
        gain_sum[1],
        finish(grad_gate),
        finish(grad_up),
        finish(grad_down_t).T,
    )


def solution(mesh):
    in_specs = (
        P(("fsdp", "ctx"), None),
        P("fsdp", None),
        P(("fsdp", "ctx"), None),
        P("fsdp"),
        P("fsdp", "tp"),
        P("fsdp", "tp"),
        P("fsdp", "tp"),
        P("tp", "fsdp"),
        P("fsdp"),
        P("fsdp", "tp"),
        P("fsdp", "tp"),
        P("tp", "fsdp"),
    )
    out_specs = (
        P(("fsdp", "ctx"), None),
        P(("fsdp", "ctx"), None),
        P(("fsdp", "ctx")),
        P(("fsdp", "ctx"), "tp"),
        P(("fsdp", "ctx"), "tp"),
        P(("fsdp", "ctx"), "tp"),
        P("tp", ("fsdp", "ctx")),
        P(("fsdp", "ctx")),
        P(("fsdp", "ctx"), "tp"),
        P(("fsdp", "ctx"), "tp"),
        P("tp", ("fsdp", "ctx")),
    )
    return jax.shard_map(shards, mesh=mesh, in_specs=in_specs, out_specs=out_specs, check_vma=False)
```
